32 devices in a mesh: node: 16 (over z, y, core), harm: 2 (over x).
Axes of the slice: x: 2, y: 2, z: 4, core: 2. Of those that a mesh axis runs over, the one named last changes fastest.
Arguments:
- spectrum: float32 [128, 3, 98304], P('harm', None, 'node'), may hold values from -2 to 2
- source: float32 [128, 3, 98304], P('harm', None, 'node'), may hold values from -4 to 4
- coupling: bfloat16 [768, 4, 128, 128], P('node'), may hold values from -0.75 to 0.75
- capacitance: float32 [98304], P('node'), may hold values from 0.5 to 4
- saturation: float32 [98304], P('node'), may hold values from 0.1 to 1
- steepness: float32 [98304], P('node'), may hold values from 0.5 to 4
- junction: float32 [98304], P('node'), may hold values from 0.2 to 2
- halo_list: int32 [16, 4, 4], replicated, may hold values from 0 to 47, as said below
- neighbour_slot: int32 [768, 4], P('node'), may hold values from 0 to 64, as said below
Outputs:
- residual: float32 [128, 3, 98304], P('harm', None, 'node')
The draws below stay inside these ranges and needn't reach their ends.
Inputs may be any that keep to these rules, and one draw needn't show every extreme that they name: `halo_list`: row [m, j] lists 4 distinct blocks of device m, by index among its 48 blocks, needed by the device at index m + o_j along node, o = (-2, -1, 1, 2). `neighbour_slot`: column 0 of block b is b's own index among the 48 blocks of its device d. Other entries v: own block v if v < 48; block halo_list[m, j, s] of device m = d - o_j if v = 48 + j * 4 + s, only where m lies on the mesh; v = 64 is an empty entry. Every such slot of a device whose sender lies on the mesh is named by some entry of the device.
All inputs are finite; a program needn't handle non-finite values.
Results may differ from the reference program's by a relative error of at most 0.0025.
Values may be sent and summed in bfloat16 or wider, within the bound.
No kernel may reach another device: no remote copies, remote signals or barrier semaphores. Data moves between devices by JAX's collectives and lax.ppermute only.
A program may use at most 128 MiB of HBM per device.

```python
import math
import jax
import jax.numpy as jnp
from jax import lax

HARMS = 64
SPEC = 128
BLK = 128
NNZ = 4
SLOTS = 4
POINTS = 3
NB_DEV = 48
NBLK = 768
NODES = 98304
N_NODE = 16


def draw_halo_list(key, part):
    keys = jax.random.split(key, N_NODE * 4)
    chosen = jax.vmap(lambda single: jax.random.permutation(single, NB_DEV)[:SLOTS])(keys)
    return chosen.reshape(N_NODE, 4, SLOTS).astype(jnp.int32)


def draw_neighbour_slot(key, part):
    empty_slot = NB_DEV + 4 * SLOTS
    entries = NB_DEV * (NNZ - 1)

    def per_device(device_key, device):
        first_key, second_key = jax.random.split(device_key)
        halo_slots = NB_DEV + jnp.arange(4 * SLOTS, dtype=jnp.int32)
        others = jax.random.randint(first_key, (entries - 4 * SLOTS,), 0, empty_slot + 1, dtype=jnp.int32)
        mixed = jax.random.permutation(second_key, jnp.concatenate([halo_slots, others]))
        direction = jnp.clip((mixed - NB_DEV) // SLOTS, 0, 3)
        offset = direction - 2 + (direction >= 2).astype(jnp.int32)
        sender = device - offset
        remote = (mixed >= NB_DEV) & (mixed < empty_slot)
        broken = remote & ((sender < 0) | (sender >= N_NODE))
        mixed = jnp.where(broken, empty_slot, mixed)
        own_column = jnp.arange(NB_DEV, dtype=jnp.int32)[:, None]
        return jnp.concatenate([own_column, mixed.reshape(NB_DEV, NNZ - 1)], axis=1)
    device_keys = jax.random.split(key, N_NODE)
    table = jax.vmap(per_device)(device_keys, jnp.arange(N_NODE, dtype=jnp.int32))
    return table.reshape(N_NODE * NB_DEV, NNZ).astype(jnp.int32)


def shard_levels(own_key, dims, cuts, least, top_value):
    factor_of = 1.0
    for dim, blocks in cuts:
        steps = jax.random.uniform(jax.random.fold_in(jax.random.fold_in(own_key, 6), dim), (blocks,), jnp.float32, least / len(cuts), top_value / len(cuts))
        factor_of = factor_of * jnp.repeat(jnp.exp(steps), dims[dim] // blocks).reshape((-1,) + (1,) * (len(dims) - 1 - dim))
    return factor_of


def centred(key, extent, spread, reach, cuts=(), kind=jnp.bfloat16):
    values = jax.random.normal(key, extent, jnp.float32) * spread
    if len(cuts) > 0:
        values = shard_levels(key, extent, cuts, -0.22, 0.18) * values
    return jnp.clip(values, min=-reach, max=reach).astype(kind)


def setup_inputs(seed: int = 0) -> dict:
    key_list = jax.random.split(jax.random.key(seed), 10)
    return {
        "spectrum": centred(key_list[0], (SPEC, POINTS, NODES), 0.15, 2.0, ((0, 2), (2, 16)), jnp.float32),
        "source": centred(key_list[1], (SPEC, POINTS, NODES), 0.3, 4.0, ((0, 2), (2, 16)), jnp.float32),
        "coupling": centred(key_list[2], (NBLK, NNZ, BLK, BLK), (NNZ * BLK // 8) ** -0.5, 0.75, ((0, 16),)),
        "capacitance": jnp.clip(jnp.exp(math.log(4.0) - 2.0794415 * jax.random.uniform(key_list[3], (NODES,), jnp.float32) ** shard_levels(key_list[3], (NODES,), ((0, 16),), -0.2, 0.2)), 0.5, 4.0),
        "saturation": jnp.clip(jnp.exp(math.log(1.0) - 2.3025851 * jax.random.uniform(key_list[4], (NODES,), jnp.float32) ** shard_levels(key_list[4], (NODES,), ((0, 16),), -0.2, 0.2)), 0.1, 1.0),
        "steepness": jnp.clip(jnp.exp(math.log(4.0) - 2.0794415 * jax.random.uniform(key_list[5], (NODES,), jnp.float32) ** shard_levels(key_list[5], (NODES,), ((0, 16),), -0.2, 0.2)), 0.5, 4.0),
        "junction": jnp.clip(jnp.exp(math.log(2.0) - 2.3025851 * jax.random.uniform(key_list[6], (NODES,), jnp.float32) ** shard_levels(key_list[6], (NODES,), ((0, 16),), -0.2, 0.2)), 0.2, 2.0),
        "halo_list": draw_halo_list(jax.random.fold_in(key_list[9], 71), 0),
        "neighbour_slot": draw_neighbour_slot(jax.random.fold_in(key_list[9], 71), 0),
    }


LOG_TWO = 0.6931471805599453

def synthesize(spectra):
    halfway = SPEC // 2
    cosines = spectra[0::2]
    sines = spectra[1::2]
    real_part = jnp.concatenate([cosines[:1] * SPEC, cosines[1:] * halfway, sines[:1] * SPEC], axis=0)
    zero_row = jnp.zeros_like(sines[:1])
    imag_part = jnp.concatenate([zero_row, -sines[1:] * halfway, zero_row], axis=0)
    return jnp.fft.irfft(real_part + 1j * imag_part, n=SPEC, axis=0).astype(jnp.float32)

def analyze(samples):
    halfway = SPEC // 2
    spectra = jnp.fft.rfft(samples, axis=0)
    lowest = spectra[0].real / SPEC
    highest = spectra[halfway].real / SPEC
    cosines = jnp.concatenate([lowest[None], 2.0 * spectra[1:halfway].real / SPEC], axis=0)
    sines = jnp.concatenate([highest[None], -2.0 * spectra[1:halfway].imag / SPEC], axis=0)
    return jnp.stack([cosines, sines], axis=1).reshape(SPEC, samples.shape[1]).astype(jnp.float32)

def derivative(spectra):
    pulsation = jnp.arange(SPEC // 2, dtype=jnp.float32)[:, None] / HARMS
    cosines = spectra[0::2]
    sines = spectra[1::2]
    return jnp.stack([pulsation * sines, -pulsation * cosines], axis=1).reshape(spectra.shape)

def single_level(spectrum, source, coupling, capacitance, saturation, steepness, junction, halo_list, neighbour_slot):
    rounded = spectrum.astype(jnp.bfloat16)
    blocks = rounded.reshape(SPEC, NBLK, BLK).transpose(1, 0, 2)
    offsets = jnp.array([-2, -1, 1, 2], dtype=jnp.int32)
    empty_slot = NB_DEV + 4 * SLOTS

    def per_device(device):
        slots = lax.dynamic_slice_in_dim(neighbour_slot, device * NB_DEV, NB_DEV, 0)
        relative = jnp.clip(slots - NB_DEV, 0, 4 * SLOTS - 1)
        direction = relative // SLOTS
        position = relative % SLOTS
        sender = jnp.clip(device - offsets[direction], 0, N_NODE - 1)
        remote = sender * NB_DEV + halo_list[sender, direction, position]
        global_id = jnp.where(slots < NB_DEV, device * NB_DEV + slots, remote)
        global_id = jnp.where(slots == empty_slot, 0, global_id).astype(jnp.int32)
        keep = (slots != empty_slot).astype(jnp.float32)
        picked = blocks[global_id].astype(jnp.float32) * keep[:, :, None, None]
        matrices = lax.dynamic_slice_in_dim(coupling, device * NB_DEV, NB_DEV, 0).astype(jnp.float32)
        return jnp.einsum('bksj,bkij->bsi', picked, matrices, precision=lax.Precision.HIGHEST)
    coupled = lax.map(per_device, jnp.arange(N_NODE, dtype=jnp.int32))
    coupled = coupled.reshape(NBLK, SPEC, BLK).transpose(1, 0, 2).reshape(SPEC, NODES)
    voltage = synthesize(spectrum)
    current = saturation * (jax.nn.softplus(steepness * voltage) - LOG_TWO)
    charge = junction * voltage / jnp.sqrt(1.0 + voltage * voltage)
    current_spec = analyze(current)
    charge_spec = analyze(charge)
    return coupled + derivative(capacitance * spectrum) + current_spec + derivative(charge_spec) - source

def reference(spectrum, source, coupling, capacitance, saturation, steepness, junction, halo_list, neighbour_slot):
    levels = []
    for level in range(POINTS):
        levels.append(single_level(spectrum[:, level], source[:, level], coupling, capacitance, saturation, steepness, junction, halo_list, neighbour_slot))
    return jnp.stack(levels, axis=1)
```

```python
import functools

import jax
import jax.numpy as jnp
import numpy as np
from jax import lax
from jax.experimental import pallas as pl
from jax.experimental.pallas import tpu as pltpu
from jax.sharding import PartitionSpec as P

LOG_TWO = 0.6931471805599453
OFFSETS = (-2, -1, 1, 2)
LANES = 128


def passed_along(value, axis, by):
    length = lax.axis_size(axis)
    pairs = [(i, i + by) for i in range(length) if 0 <= i + by < length]
    return lax.ppermute(value, axis, pairs)


def passed_round(value, axis, by):
    length = lax.axis_size(axis)
    return lax.ppermute(value, axis, [(i, (i + by) % length) for i in range(length)])


def tables(rows, parts):
    length = rows * parts
    harmonics = length // 2
    sample = np.arange(length)[:, None]
    column = np.arange(length)[None, :]
    angle = 2.0 * np.pi / length * (column // 2 * sample % length)
    synthesis = np.where(column % 2 == 1, np.sin(angle), np.cos(angle))
    synthesis[:, 1] = np.where(sample[:, 0] % 2 == 0, 1.0, -1.0)
    weights = np.where(np.arange(length) < 2, 1.0, 2.0) / length
    analysis = synthesis.T * weights[:, None]
    order = np.arange(length)
    pulsation = np.where(order % 2 == 0, 1.0, -1.0) * (order // 2) / harmonics
    derived = analysis[order ^ 1] * pulsation[:, None]
    arrive = [
        np.concatenate(
            [synthesis[:, (h - s) % parts * rows :][:, :rows] for s in range(parts)], axis=1
        )
        for h in range(parts)
    ]
    return (
        np.stack(arrive),
        analysis.reshape(parts, rows, length),
        derived.reshape(parts, rows, length),
        np.broadcast_to(pulsation[:, None], (length, LANES)).reshape(parts, rows, LANES),
    )


def pack_kernel(index_ref, *refs):
    points = len(refs) - len(OFFSETS)
    slots = index_ref.shape[0] // len(OFFSETS)
    size = refs[-1].shape[-1] // slots
    for d in range(len(OFFSETS)):
        for s in range(slots):
            start = pl.multiple_of(index_ref[d * slots + s] * size, size)
            for p in range(points):
                refs[points + d][p, :, s * size : (s + 1) * size] = refs[p][:, pl.ds(start, size)]


def coupled_kernel(
    per_step, points, slot_ref, h_ref, *refs
):
    owns = refs[:points]
    halos = refs[points : points + len(OFFSETS)]
    (coupling, spectrum, source, capacitance, pulsation, out, blocks) = refs[
        points + len(OFFSETS) :
    ]
    rows, nodes = owns[0].shape
    listed = coupling.shape[1]
    size = coupling.shape[2]
    count = nodes // size
    slots = halos[0].shape[-1] // size

    @pl.when(pl.program_id(0) == 0)
    def _():
        for p in range(points):
            at = slice(p * rows, (p + 1) * rows)
            for b in range(count):
                blocks[b, at, :] = owns[p][:, b * size : (b + 1) * size]
            for d in range(len(OFFSETS)):
                for s in range(slots):
                    blocks[count + d * slots + s, at, :] = halos[d][
                        p, :, s * size : (s + 1) * size
                    ]
        blocks[count + len(OFFSETS) * slots] = jnp.zeros(blocks.shape[1:], blocks.dtype)

    even = lax.broadcasted_iota(jnp.int32, (rows, size), 0) % 2 == 0
    for b in range(per_step):
        entry = (pl.program_id(0) * per_step + b) * listed
        left = jnp.concatenate([blocks[slot_ref[entry + k]] for k in range(listed)], axis=1)
        right = jnp.concatenate([coupling[b, k] for k in range(listed)], axis=1)
        total = lax.dot_general(
            left, right, (((1,), (1,)), ((), ())), preferred_element_type=jnp.float32
        )
        at = slice(b * size, (b + 1) * size)
        scale = pulsation[0] * capacitance[:, at]
        for p in range(points):
            values = spectrum[p, :, at]
            swapped = jnp.where(
                even, pltpu.roll(values, rows - 1, 0), pltpu.roll(values, 1, 0)
            )
            out[p, :, at] = (
                total[p * rows : (p + 1) * rows] + scale * swapped - source[p, :, at]
            )


def nonlinear_kernel(parts, width, h_ref, *refs):
    arrived = refs[:parts]
    (base, saturation, steepness, junction, synthesis, analysis, derived, out) = refs[parts:]
    for start in range(0, out.shape[-1], width):
        at = slice(start, start + width)
        spectra = jnp.concatenate([ref[:, at] for ref in arrived], axis=0)
        voltage = jnp.dot(synthesis[0], spectra, preferred_element_type=jnp.float32)
        u = steepness[:, at] * voltage
        current = jnp.maximum(u, 0.0) + jnp.log(1.0 + jnp.exp(-jnp.abs(u))) - LOG_TWO
        charge = voltage * lax.rsqrt(1.0 + voltage * voltage)
        first = jnp.dot(
            analysis[0], current.astype(jnp.bfloat16), preferred_element_type=jnp.float32
        )
        second = jnp.dot(
            derived[0], charge.astype(jnp.bfloat16), preferred_element_type=jnp.float32
        )
        out[0, :, at] = (
            base[0, :, at] + saturation[:, at] * first + junction[:, at] * second
        )


def widest(total, unit, most):
    return max(w for w in range(unit, most + 1, unit) if total % w == 0)


def local(
    spectrum,
    source,
    coupling,
    capacitance,
    saturation,
    steepness,
    junction,
    halo_list,
    neighbour_slot,
):
    rows, points, nodes = spectrum.shape
    parts = lax.axis_size("harm")
    length = rows * parts
    count, listed, size, _ = coupling.shape
    slots = halo_list.shape[-1]
    harm = lax.axis_index("harm").astype(jnp.int32).reshape(1)
    synthesis, analysis, derived, pulsation = tables(rows, parts)
    synthesis = jnp.asarray(synthesis, jnp.bfloat16)
    analysis = jnp.asarray(analysis, jnp.bfloat16)
    derived = jnp.asarray(derived, jnp.bfloat16)
    pulsation = jnp.asarray(pulsation, jnp.float32)

    by_point = spectrum.transpose(1, 0, 2)
    source_by_point = source.transpose(1, 0, 2)
    owns = [by_point[p].astype(jnp.bfloat16) for p in range(points)]
    arrived = [
        [own] + [passed_round(own, "harm", s) for s in range(1, parts)] for own in owns
    ]

    wanted = halo_list[lax.axis_index("node")].reshape(-1)
    vmem = pl.BlockSpec(memory_space=pltpu.VMEM)
    packed = pl.pallas_call(
        pack_kernel,
        out_shape=[jax.ShapeDtypeStruct((points, rows, slots * size), jnp.bfloat16)]
        * len(OFFSETS),
        in_specs=[pl.BlockSpec(memory_space=pltpu.SMEM)] + [vmem] * points,
        out_specs=[vmem] * len(OFFSETS),
        name="pack",
    )(wanted, *owns)
    halos = [passed_along(value, "node", offset) for value, offset in zip(packed, OFFSETS)]

    per_step = widest(count, 1, 4)
    wide = per_step * size
    base = pl.pallas_call(
        functools.partial(coupled_kernel, per_step, points),
        out_shape=jax.ShapeDtypeStruct((points, rows, nodes), jnp.float32),
        grid_spec=pltpu.PrefetchScalarGridSpec(
            num_scalar_prefetch=2,
            grid=(count // per_step,),
            in_specs=[pl.BlockSpec((rows, nodes), lambda i, n, h: (0, 0))] * points
            + [pl.BlockSpec((points, rows, slots * size), lambda i, n, h: (0, 0, 0))]
            * len(OFFSETS)
            + [
                pl.BlockSpec((per_step, listed, size, size), lambda i, n, h: (i, 0, 0, 0)),
                pl.BlockSpec((points, rows, wide), lambda i, n, h: (0, 0, i)),
                pl.BlockSpec((points, rows, wide), lambda i, n, h: (0, 0, i)),
                pl.BlockSpec((1, wide), lambda i, n, h: (0, i)),
                pl.BlockSpec((1, rows, LANES), lambda i, n, h: (h[0], 0, 0)),
            ],
            out_specs=pl.BlockSpec((points, rows, wide), lambda i, n, h: (0, 0, i)),
            scratch_shapes=[
                pltpu.VMEM((count + len(OFFSETS) * slots + 1, points * rows, size), jnp.bfloat16)
            ],
        ),
        cost_estimate=pl.CostEstimate(
            flops=2 * points * rows * nodes * listed * size,
            bytes_accessed=coupling.size * 2 + spectrum.size * 14,
            transcendentals=0,
        ),
        name="coupled",
    )(
        neighbour_slot.reshape(-1),
        harm,
        *owns,
        *halos,
        coupling,
        by_point,
        source_by_point,
        capacitance.reshape(1, -1),
        pulsation,
    )

    block = widest(nodes, LANES, 1536)
    width = widest(block, LANES, 256)
    result = base
    for p in range(points):
        table = pl.BlockSpec((1, length, length), lambda i, h: (h[0], 0, 0))
        half = pl.BlockSpec((1, rows, length), lambda i, h: (h[0], 0, 0))
        whole = pl.BlockSpec((1, rows, block), lambda i, h, p=p: (p, 0, i))
        scale = pl.BlockSpec((1, block), lambda i, h: (0, i))
        result = pl.pallas_call(
            functools.partial(nonlinear_kernel, parts, width),
            out_shape=jax.ShapeDtypeStruct(base.shape, base.dtype),
            grid_spec=pltpu.PrefetchScalarGridSpec(
                num_scalar_prefetch=1,
                grid=(nodes // block,),
                in_specs=[pl.BlockSpec((rows, block), lambda i, h: (0, i))] * parts
                + [whole]
                + [scale] * 3
                + [table, half, half],
                out_specs=whole,
            ),
            input_output_aliases={1 + parts: 0},
            cost_estimate=pl.CostEstimate(
                flops=2 * (length + 2 * rows) * length * nodes,
                bytes_accessed=12 * rows * nodes,
                transcendentals=3 * length * nodes,
            ),
            name="nonlinear",
        )(
            harm,
            *arrived[p],
            result,
            saturation.reshape(1, -1),
            steepness.reshape(1, -1),
            junction.reshape(1, -1),
            synthesis,
            analysis,
            derived,
        )
    return result.transpose(1, 0, 2)


def solution(mesh):
    in_specs = (
        P("harm", None, "node"),
        P("harm", None, "node"),
        P("node", None, None, None),
        P("node"),
        P("node"),
        P("node"),
        P("node"),
        P(),
        P("node", None),
    )
    out_specs = P("harm", None, "node")
    return jax.shard_map(local, mesh=mesh, in_specs=in_specs, out_specs=out_specs, check_vma=False)
```

```python
import functools

import jax
import jax.numpy as jnp
import numpy as np
from jax import lax
from jax.experimental import pallas as pl
from jax.experimental.pallas import tpu as pltpu
from jax.sharding import PartitionSpec as P

LOG_TWO = 0.6931471805599453
OFFSETS = (-2, -1, 1, 2)
LANES = 128


def passed_along(value, axis, by):
    length = lax.axis_size(axis)
    pairs = [(i, i + by) for i in range(length) if 0 <= i + by < length]
    return lax.ppermute(value, axis, pairs)


def passed_round(value, axis, by):
    length = lax.axis_size(axis)
    return lax.ppermute(value, axis, [(i, (i + by) % length) for i in range(length)])


def tables(rows, parts):
    length = rows * parts
    harmonics = length // 2
    sample = np.arange(length)[:, None]
    column = np.arange(length)[None, :]
    angle = 2.0 * np.pi / length * (column // 2 * sample % length)
    synthesis = np.where(column % 2 == 1, np.sin(angle), np.cos(angle))
    synthesis[:, 1] = np.where(sample[:, 0] % 2 == 0, 1.0, -1.0)
    weights = np.where(np.arange(length) < 2, 1.0, 2.0) / length
    analysis = synthesis.T * weights[:, None]
    order = np.arange(length)
    pulsation = np.where(order % 2 == 0, 1.0, -1.0) * (order // 2) / harmonics
    derived = analysis[order ^ 1] * pulsation[:, None]
    arrive = [
        np.concatenate(
            [synthesis[:, (h - s) % parts * rows :][:, :rows] for s in range(parts)], axis=1
        )
        for h in range(parts)
    ]
    return (
        np.stack(arrive),
        analysis.reshape(parts, rows, length),
        derived.reshape(parts, rows, length),
        np.broadcast_to(pulsation[:, None], (length, LANES)).reshape(parts, rows, LANES),
    )


def round_kernel(spectrum, out):
    out[...] = spectrum[0].astype(out.dtype)


def pack_kernel(node_ref, halo_ref, spectrum, *refs):
    outs = refs[: len(OFFSETS)]
    landed, done = refs[len(OFFSETS) :]
    slots = halo_ref.shape[1]
    size = outs[0].shape[-1] // slots
    copies = []
    for d in range(len(OFFSETS)):
        for s in range(slots):
            start = pl.multiple_of(halo_ref[d, s, node_ref[0]] * size, size)
            copy = pltpu.make_async_copy(
                spectrum.at[:, :, pl.ds(start, size)],
                landed.at[d * slots + s],
                done.at[d * slots + s],
            )
            copy.start()
            copies.append(copy)
    for d in range(len(OFFSETS)):
        for s in range(slots):
            copies[d * slots + s].wait()
            outs[d][:, :, s * size : (s + 1) * size] = landed[d * slots + s].astype(
                outs[d].dtype
            )


def coupled_kernel(per_step, points, chunks, slot_ref, h_ref, *refs):
    owns = refs[: len(chunks)]
    halos = refs[len(chunks) : len(chunks) + len(OFFSETS)]
    (coupling, spectrum, source, capacitance, pulsation, out, blocks) = refs[
        len(chunks) + len(OFFSETS) :
    ]
    rows = owns[0].shape[0]
    listed = coupling.shape[1]
    size = coupling.shape[2]
    slots = halos[0].shape[-1] // size
    count = blocks.shape[0] - len(OFFSETS) * slots - 1

    @pl.when(pl.program_id(0) == 0)
    def _():
        for (p, begin, wide), own in zip(chunks, owns):
            at = slice(p * rows, (p + 1) * rows)
            for b in range(wide // size):
                blocks[begin // size + b, at, :] = own[:, b * size : (b + 1) * size]
        for p in range(points):
            at = slice(p * rows, (p + 1) * rows)
            for d in range(len(OFFSETS)):
                for s in range(slots):
                    blocks[count + d * slots + s, at, :] = halos[d][
                        p, :, s * size : (s + 1) * size
                    ]
        blocks[count + len(OFFSETS) * slots] = jnp.zeros(blocks.shape[1:], blocks.dtype)

    even = lax.broadcasted_iota(jnp.int32, (rows, size), 0) % 2 == 0
    for b in range(per_step):
        entry = pl.program_id(0) * per_step + b
        left = jnp.concatenate([blocks[slot_ref[k, entry]] for k in range(listed)], axis=1)
        right = jnp.concatenate([coupling[b, k] for k in range(listed)], axis=1)
        total = lax.dot_general(
            left, right, (((1,), (1,)), ((), ())), preferred_element_type=jnp.float32
        )
        at = slice(b * size, (b + 1) * size)
        scale = pulsation[0] * capacitance[:, at]
        for p in range(points):
            values = spectrum[p, :, at]
            swapped = jnp.where(
                even, pltpu.roll(values, rows - 1, 0), pltpu.roll(values, 1, 0)
            )
            out[p, :, at] = (
                total[p * rows : (p + 1) * rows] + scale * swapped - source[p, :, at]
            )


def nonlinear_kernel(parts, width, h_ref, *refs):
    arrived = refs[:parts]
    (base, saturation, steepness, junction, synthesis, analysis, derived, out) = refs[parts:]
    for start in range(0, out.shape[-1], width):
        at = slice(start, start + width)
        spectra = jnp.concatenate([ref[:, at] for ref in arrived], axis=0)
        voltage = jnp.dot(synthesis[0], spectra, preferred_element_type=jnp.float32)
        u = steepness[:, at] * voltage
        current = jnp.maximum(u, 0.0) + jnp.log(1.0 + jnp.exp(-jnp.abs(u))) - LOG_TWO
        charge = voltage * lax.rsqrt(1.0 + voltage * voltage)
        first = jnp.dot(
            analysis[0], current.astype(jnp.bfloat16), preferred_element_type=jnp.float32
        )
        second = jnp.dot(
            derived[0], charge.astype(jnp.bfloat16), preferred_element_type=jnp.float32
        )
        out[0, :, at] = (
            base[0, :, at] + saturation[:, at] * first + junction[:, at] * second
        )


def widest(total, unit, most):
    return max(w for w in range(unit, most + 1, unit) if total % w == 0)


def local(
    spectrum,
    source,
    coupling,
    capacitance,
    saturation,
    steepness,
    junction,
    halo_list,
    neighbour_slot,
):
    rows, points, nodes = spectrum.shape
    parts = lax.axis_size("harm")
    length = rows * parts
    count, listed, size, _ = coupling.shape
    slots = halo_list.shape[-1]
    harm = lax.axis_index("harm").astype(jnp.int32).reshape(1)
    synthesis, analysis, derived, pulsation = tables(rows, parts)
    synthesis = jnp.asarray(synthesis, jnp.bfloat16)
    analysis = jnp.asarray(analysis, jnp.bfloat16)
    derived = jnp.asarray(derived, jnp.bfloat16)
    pulsation = jnp.asarray(pulsation, jnp.float32)

    by_point = spectrum.transpose(1, 0, 2)
    source_by_point = source.transpose(1, 0, 2)
    block = widest(nodes, LANES, 1536)
    chunks = [(p, 0, nodes) for p in range(points)]
    if nodes > block:
        chunks[-1:] = [(points - 1, 0, nodes - block), (points - 1, nodes - block, block)]
    owns = []
    for p, begin, wide in chunks:
        owns.append(
            pl.pallas_call(
                round_kernel,
                out_shape=jax.ShapeDtypeStruct((rows, wide), jnp.bfloat16),
                grid=(wide // block,),
                in_specs=[
                    pl.BlockSpec(
                        (1, rows, block), lambda i, p=p, j=begin // block: (p, 0, i + j)
                    )
                ],
                out_specs=pl.BlockSpec((rows, block), lambda i: (0, i)),
                name="rounded",
            )(by_point)
        )
    arrived = [
        [own] + [passed_round(own, "harm", s) for s in range(1, parts)] for own in owns
    ]

    smem = pl.BlockSpec(memory_space=pltpu.SMEM)
    vmem = pl.BlockSpec(memory_space=pltpu.VMEM)
    packed = pl.pallas_call(
        pack_kernel,
        out_shape=[jax.ShapeDtypeStruct((points, rows, slots * size), jnp.bfloat16)]
        * len(OFFSETS),
        in_specs=[smem, smem, pl.BlockSpec(memory_space=pl.ANY)],
        out_specs=[vmem] * len(OFFSETS),
        scratch_shapes=[
            pltpu.VMEM((len(OFFSETS) * slots, points, rows, size), jnp.float32),
            pltpu.SemaphoreType.DMA((len(OFFSETS) * slots,)),
        ],
        name="pack",
    )(
        lax.axis_index("node").astype(jnp.int32).reshape(1),
        halo_list.transpose(1, 2, 0),
        by_point,
    )
    halos = [passed_along(value, "node", offset) for value, offset in zip(packed, OFFSETS)]

    per_step = widest(count, 1, 8)
    span = per_step * size
    base = pl.pallas_call(
        functools.partial(coupled_kernel, per_step, points, chunks),
        out_shape=jax.ShapeDtypeStruct((points, rows, nodes), jnp.float32),
        grid_spec=pltpu.PrefetchScalarGridSpec(
            num_scalar_prefetch=2,
            grid=(count // per_step,),
            in_specs=[pl.BlockSpec(own.shape, lambda i, n, h: (0, 0)) for own in owns]
            + [pl.BlockSpec((points, rows, slots * size), lambda i, n, h: (0, 0, 0))]
            * len(OFFSETS)
            + [
                pl.BlockSpec((per_step, listed, size, size), lambda i, n, h: (i, 0, 0, 0)),
                pl.BlockSpec((points, rows, span), lambda i, n, h: (0, 0, i)),
                pl.BlockSpec((points, rows, span), lambda i, n, h: (0, 0, i)),
                pl.BlockSpec((1, span), lambda i, n, h: (0, i)),
                pl.BlockSpec((1, rows, LANES), lambda i, n, h: (h[0], 0, 0)),
            ],
            out_specs=pl.BlockSpec((points, rows, span), lambda i, n, h: (0, 0, i)),
            scratch_shapes=[
                pltpu.VMEM((count + len(OFFSETS) * slots + 1, points * rows, size), jnp.bfloat16)
            ],
        ),
        cost_estimate=pl.CostEstimate(
            flops=2 * points * rows * nodes * listed * size,
            bytes_accessed=coupling.size * 2 + spectrum.size * 14,
            transcendentals=0,
        ),
        name="coupled",
    )(
        neighbour_slot.T,
        harm,
        *owns,
        *halos,
        coupling,
        by_point,
        source_by_point,
        capacitance.reshape(1, -1),
        pulsation,
    )

    width = widest(block, LANES, 256)
    result = base
    for (p, begin, wide), pair in zip(chunks, arrived):
        at = begin // block
        table = pl.BlockSpec((1, length, length), lambda i, h: (h[0], 0, 0))
        half = pl.BlockSpec((1, rows, length), lambda i, h: (h[0], 0, 0))
        whole = pl.BlockSpec((1, rows, block), lambda i, h, p=p, j=at: (p, 0, i + j))
        scale = pl.BlockSpec((1, block), lambda i, h, j=at: (0, i + j))
        result = pl.pallas_call(
            functools.partial(nonlinear_kernel, parts, width),
            out_shape=jax.ShapeDtypeStruct(base.shape, base.dtype),
            grid_spec=pltpu.PrefetchScalarGridSpec(
                num_scalar_prefetch=1,
                grid=(wide // block,),
                in_specs=[pl.BlockSpec((rows, block), lambda i, h: (0, i))] * parts
                + [whole]
                + [scale] * 3
                + [table, half, half],
                out_specs=whole,
            ),
            input_output_aliases={1 + parts: 0},
            cost_estimate=pl.CostEstimate(
                flops=2 * (length + 2 * rows) * length * wide,
                bytes_accessed=12 * rows * wide,
                transcendentals=3 * length * wide,
            ),
            name="nonlinear",
        )(
            harm,
            *pair,
            result,
            saturation.reshape(1, -1),
            steepness.reshape(1, -1),
            junction.reshape(1, -1),
            synthesis,
            analysis,
            derived,
        )
    return result.transpose(1, 0, 2)


def solution(mesh):
    in_specs = (
        P("harm", None, "node"),
        P("harm", None, "node"),
        P("node", None, None, None),
        P("node"),
        P("node"),
        P("node"),
        P("node"),
        P(),
        P("node", None),
    )
    out_specs = P("harm", None, "node")
    return jax.shard_map(local, mesh=mesh, in_specs=in_specs, out_specs=out_specs, check_vma=False)
```

```python
import functools

import jax
import jax.numpy as jnp
import numpy as np
from jax import lax
from jax.experimental import pallas as pl
from jax.experimental.pallas import tpu as pltpu
from jax.sharding import PartitionSpec as P

LOG_TWO = 0.6931471805599453
OFFSETS = (-2, -1, 1, 2)
LANES = 128


def passed_along(value, axis, by):
    length = lax.axis_size(axis)
    pairs = [(i, i + by) for i in range(length) if 0 <= i + by < length]
    return lax.ppermute(value, axis, pairs)


def passed_round(value, axis, by):
    length = lax.axis_size(axis)
    return lax.ppermute(value, axis, [(i, (i + by) % length) for i in range(length)])


def tables(rows, parts):
    length = rows * parts
    harmonics = length // 2
    sample = np.arange(length)[:, None]
    column = np.arange(length)[None, :]
    angle = 2.0 * np.pi / length * (column // 2 * sample % length)
    synthesis = np.where(column % 2 == 1, np.sin(angle), np.cos(angle))
    synthesis[:, 1] = np.where(sample[:, 0] % 2 == 0, 1.0, -1.0)
    weights = np.where(np.arange(length) < 2, 1.0, 2.0) / length
    analysis = synthesis.T * weights[:, None]
    order = np.arange(length)
    pulsation = np.where(order % 2 == 0, 1.0, -1.0) * (order // 2) / harmonics
    derived = analysis[order ^ 1] * pulsation[:, None]
    arrive = [
        np.concatenate(
            [synthesis[:, (h - s) % parts * rows :][:, :rows] for s in range(parts)], axis=1
        )
        for h in range(parts)
    ]
    return (
        np.stack(arrive),
        np.concatenate([analysis, derived], axis=1).reshape(parts, rows, 2 * length),
        np.broadcast_to(pulsation[:, None], (length, LANES)).reshape(parts, rows, LANES),
    )


def pack_kernel(node_ref, halo_ref, spectrum, *refs):
    outs = refs[: len(OFFSETS)]
    landed, done = refs[len(OFFSETS) :]
    slots = halo_ref.shape[1]
    size = outs[0].shape[-1] // slots
    copies = []
    for d in range(len(OFFSETS)):
        for s in range(slots):
            start = pl.multiple_of(halo_ref[d, s, node_ref[0]] * size, size)
            copy = pltpu.make_async_copy(
                spectrum.at[:, :, pl.ds(start, size)],
                landed.at[d * slots + s],
                done.at[d * slots + s],
            )
            copy.start()
            copies.append(copy)
    for d in range(len(OFFSETS)):
        for s in range(slots):
            copies[d * slots + s].wait()
            outs[d][:, :, s * size : (s + 1) * size] = landed[d * slots + s].astype(
                outs[d].dtype
            )


def coupled_kernel(per_step, points, chunks, slot_ref, h_ref, *refs):
    owns = refs[: len(chunks)]
    halos = refs[len(chunks) : len(chunks) + len(OFFSETS)]
    (coupling, spectrum, source, capacitance, pulsation, out, blocks) = refs[
        len(chunks) + len(OFFSETS) :
    ]
    rows = owns[0].shape[0]
    listed = coupling.shape[1]
    size = coupling.shape[2]
    slots = halos[0].shape[-1] // size
    count = blocks.shape[0] - len(OFFSETS) * slots - 1

    @pl.when(pl.program_id(0) == 0)
    def _():
        for (p, begin, wide), own in zip(chunks, owns):
            at = slice(p * rows, (p + 1) * rows)
            for b in range(wide // size):
                blocks[begin // size + b, at, :] = own[:, b * size : (b + 1) * size]
        for p in range(points):
            at = slice(p * rows, (p + 1) * rows)
            for d in range(len(OFFSETS)):
                for s in range(slots):
                    blocks[count + d * slots + s, at, :] = halos[d][
                        p, :, s * size : (s + 1) * size
                    ]
        blocks[count + len(OFFSETS) * slots] = jnp.zeros(blocks.shape[1:], blocks.dtype)

    even = lax.broadcasted_iota(jnp.int32, (rows, size), 0) % 2 == 0
    for b in range(per_step):
        entry = pl.program_id(0) * per_step + b
        left = jnp.concatenate([blocks[slot_ref[k, entry]] for k in range(listed)], axis=1)
        right = jnp.concatenate([coupling[b, k] for k in range(listed)], axis=1)
        total = lax.dot_general(
            left, right, (((1,), (1,)), ((), ())), preferred_element_type=jnp.float32
        )
        at = slice(b * size, (b + 1) * size)
        scale = pulsation[0] * capacitance[:, at]
        for p in range(points):
            values = spectrum[p, :, at]
            swapped = jnp.where(
                even, pltpu.roll(values, rows - 1, 0), pltpu.roll(values, 1, 0)
            )
            out[p, :, at] = (
                total[p * rows : (p + 1) * rows] + scale * swapped - source[p, :, at]
            )


def nonlinear_kernel(parts, width, h_ref, *refs):
    own = refs[0]
    others = refs[1:parts]
    (base, saturation, steepness, junction, synthesis, analysis, out) = refs[parts : parts + 7]
    (landed, done, volt, samples) = refs[parts + 7 :]
    block = out.shape[-1]
    steps = landed.shape[1]

    def copy(part, step):
        return pltpu.make_async_copy(
            others[part].at[:, step * block : (step + 1) * block],
            landed.at[part, step],
            done.at[part, step],
        )

    for step in range(steps):

        @pl.when(pl.program_id(0) == 0)
        def _():
            for part in range(parts - 1):
                copy(part, step).start()

    for step in range(steps):

        @pl.when(pl.program_id(0) == step)
        def _():
            for part in range(parts - 1):
                copy(part, step).wait()

    now = pl.program_id(0)
    length = volt.shape[1]
    group = 16
    for turn, start in enumerate(range(0, block, width)):
        at = slice(start, start + width)
        slot = turn % 2
        spectra = jnp.concatenate(
            [own[:, at]] + [landed[part, now, :, at] for part in range(parts - 1)], axis=0
        )
        volt[slot] = jnp.dot(synthesis[0], spectra, preferred_element_type=jnp.float32)
        steep = steepness[:, at]
        for row in range(0, length, group):
            here = slice(row, row + group)
            voltage = volt[slot, here, :]
            u = steep * voltage
            current = jnp.maximum(u, 0.0) + jnp.log(1.0 + jnp.exp(-jnp.abs(u))) - LOG_TWO
            samples[slot, here, :] = (saturation[:, at] * current).astype(jnp.bfloat16)
            charge = junction[:, at] * voltage * lax.rsqrt(1.0 + voltage * voltage)
            samples[slot, length + row : length + row + group, :] = charge.astype(jnp.bfloat16)
        out[0, :, at] = base[0, :, at] + jnp.dot(
            analysis[0], samples[slot], preferred_element_type=jnp.float32
        )


def widest(total, unit, most):
    return max(w for w in range(unit, most + 1, unit) if total % w == 0)


def local(
    spectrum,
    source,
    coupling,
    capacitance,
    saturation,
    steepness,
    junction,
    halo_list,
    neighbour_slot,
):
    rows, points, nodes = spectrum.shape
    parts = lax.axis_size("harm")
    length = rows * parts
    count, listed, size, _ = coupling.shape
    slots = halo_list.shape[-1]
    harm = lax.axis_index("harm").astype(jnp.int32).reshape(1)
    synthesis, analysis, pulsation = tables(rows, parts)
    synthesis = jnp.asarray(synthesis, jnp.bfloat16)
    analysis = jnp.asarray(analysis, jnp.bfloat16)
    pulsation = jnp.asarray(pulsation, jnp.float32)

    by_point = spectrum.transpose(1, 0, 2)
    source_by_point = source.transpose(1, 0, 2)
    block = widest(nodes, LANES, 1536)
    chunks = [(p, 0, nodes) for p in range(points)]
    if nodes > block:
        chunks[-1:] = [(points - 1, 0, nodes - block), (points - 1, nodes - block, block)]
    head = by_point[0].astype(jnp.bfloat16)
    later, _ = lax.optimization_barrier((by_point, head))
    owns = [head] + [
        later[p, :, begin : begin + wide].astype(jnp.bfloat16) for p, begin, wide in chunks[1:]
    ]
    after = lax.optimization_barrier((by_point, *owns))[0]
    arrived = [
        [own] + [passed_round(own, "harm", s) for s in range(1, parts)] for own in owns
    ]

    smem = pl.BlockSpec(memory_space=pltpu.SMEM)
    vmem = pl.BlockSpec(memory_space=pltpu.VMEM)
    packed = pl.pallas_call(
        pack_kernel,
        out_shape=[jax.ShapeDtypeStruct((points, rows, slots * size), jnp.bfloat16)]
        * len(OFFSETS),
        in_specs=[smem, smem, pl.BlockSpec(memory_space=pl.ANY)],
        out_specs=[vmem] * len(OFFSETS),
        scratch_shapes=[
            pltpu.VMEM((len(OFFSETS) * slots, points, rows, size), jnp.float32),
            pltpu.SemaphoreType.DMA((len(OFFSETS) * slots,)),
        ],
        name="pack",
    )(
        lax.axis_index("node").astype(jnp.int32).reshape(1),
        halo_list.transpose(1, 2, 0),
        after,
    )
    halos = [passed_along(value, "node", offset) for value, offset in zip(packed, OFFSETS)]

    per_step = widest(count, 1, 8)
    span = per_step * size
    base = pl.pallas_call(
        functools.partial(coupled_kernel, per_step, points, chunks),
        out_shape=jax.ShapeDtypeStruct((points, rows, nodes), jnp.float32),
        grid_spec=pltpu.PrefetchScalarGridSpec(
            num_scalar_prefetch=2,
            grid=(count // per_step,),
            in_specs=[pl.BlockSpec(own.shape, lambda i, n, h: (0, 0)) for own in owns]
            + [pl.BlockSpec((points, rows, slots * size), lambda i, n, h: (0, 0, 0))]
            * len(OFFSETS)
            + [
                pl.BlockSpec((per_step, listed, size, size), lambda i, n, h: (i, 0, 0, 0)),
                pl.BlockSpec((points, rows, span), lambda i, n, h: (0, 0, i)),
                pl.BlockSpec((points, rows, span), lambda i, n, h: (0, 0, i)),
                pl.BlockSpec((1, span), lambda i, n, h: (0, i)),
                pl.BlockSpec((1, rows, LANES), lambda i, n, h: (h[0], 0, 0)),
            ],
            out_specs=pl.BlockSpec((points, rows, span), lambda i, n, h: (0, 0, i)),
            scratch_shapes=[
                pltpu.VMEM((count + len(OFFSETS) * slots + 1, points * rows, size), jnp.bfloat16)
            ],
        ),
        cost_estimate=pl.CostEstimate(
            flops=2 * points * rows * nodes * listed * size,
            bytes_accessed=coupling.size * 2 + spectrum.size * 14,
            transcendentals=0,
        ),
        name="coupled",
    )(
        neighbour_slot.T,
        harm,
        *owns,
        *halos,
        coupling,
        by_point,
        source_by_point,
        capacitance.reshape(1, -1),
        pulsation,
    )

    width = widest(block, LANES, 256)
    result = base
    for (p, begin, wide), pair in zip(chunks, arrived):
        at = begin // block
        table = pl.BlockSpec((1, length, length), lambda i, h: (h[0], 0, 0))
        half = pl.BlockSpec((1, rows, 2 * length), lambda i, h: (h[0], 0, 0))
        whole = pl.BlockSpec((1, rows, block), lambda i, h, p=p, j=at: (p, 0, i + j))
        scale = pl.BlockSpec((1, block), lambda i, h, j=at: (0, i + j))
        result = pl.pallas_call(
            functools.partial(nonlinear_kernel, parts, width),
            out_shape=jax.ShapeDtypeStruct(base.shape, base.dtype),
            grid_spec=pltpu.PrefetchScalarGridSpec(
                num_scalar_prefetch=1,
                grid=(wide // block,),
                in_specs=[pl.BlockSpec((rows, block), lambda i, h: (0, i))]
                + [pl.BlockSpec(memory_space=pl.ANY)] * (parts - 1)
                + [whole]
                + [scale] * 3
                + [table, half],
                out_specs=whole,
                scratch_shapes=[
                    pltpu.VMEM((parts - 1, wide // block, rows, block), jnp.bfloat16),
                    pltpu.SemaphoreType.DMA((parts - 1, wide // block)),
                    pltpu.VMEM((2, length, width), jnp.float32),
                    pltpu.VMEM((2, 2 * length, width), jnp.bfloat16),
                ],
            ),
            input_output_aliases={1 + parts: 0},
            cost_estimate=pl.CostEstimate(
                flops=2 * (length + 2 * rows) * length * wide,
                bytes_accessed=12 * rows * wide,
                transcendentals=3 * length * wide,
            ),
            name="nonlinear",
        )(
            harm,
            *pair,
            result,
            saturation.reshape(1, -1),
            steepness.reshape(1, -1),
            junction.reshape(1, -1),
            synthesis,
            analysis,
        )
    return result.transpose(1, 0, 2)


def solution(mesh):
    in_specs = (
        P("harm", None, "node"),
        P("harm", None, "node"),
        P("node", None, None, None),
        P("node"),
        P("node"),
        P("node"),
        P("node"),
        P(),
        P("node", None),
    )
    out_specs = P("harm", None, "node")
    return jax.shard_map(local, mesh=mesh, in_specs=in_specs, out_specs=out_specs, check_vma=False)
```

```python
import functools

import jax
import jax.numpy as jnp
import numpy as np
from jax import lax
from jax.experimental import pallas as pl
from jax.experimental.pallas import tpu as pltpu
from jax.sharding import PartitionSpec as P

LOG_TWO = 0.6931471805599453
OFFSETS = (-2, -1, 1, 2)
LANES = 128


def passed_along(value, axis, by):
    length = lax.axis_size(axis)
    pairs = [(i, i + by) for i in range(length) if 0 <= i + by < length]
    return lax.ppermute(value, axis, pairs)


def passed_round(value, axis, by):
    length = lax.axis_size(axis)
    return lax.ppermute(value, axis, [(i, (i + by) % length) for i in range(length)])


def tables(rows, parts):
    length = rows * parts
    harmonics = length // 2
    sample = np.arange(length)[:, None]
    column = np.arange(length)[None, :]
    angle = 2.0 * np.pi / length * (column // 2 * sample % length)
    synthesis = np.where(column % 2 == 1, np.sin(angle), np.cos(angle))
    synthesis[:, 1] = np.where(sample[:, 0] % 2 == 0, 1.0, -1.0)
    weights = np.where(np.arange(length) < 2, 1.0, 2.0) / length
    analysis = synthesis.T * weights[:, None]
    order = np.arange(length)
    pulsation = np.where(order % 2 == 0, 1.0, -1.0) * (order // 2) / harmonics
    derived = analysis[order ^ 1] * pulsation[:, None]
    arrive = [
        np.concatenate(
            [synthesis[:, (h - s) % parts * rows :][:, :rows] for s in range(parts)], axis=1
        )
        for h in range(parts)
    ]
    return (
        np.stack(arrive),
        np.concatenate([analysis, derived], axis=1).reshape(parts, rows, 2 * length),
        np.broadcast_to(pulsation[:, None], (length, LANES)).reshape(parts, rows, LANES),
    )


def pack_kernel(node_ref, halo_ref, spectrum, *refs):
    outs = refs[: len(OFFSETS)]
    landed, done = refs[len(OFFSETS) :]
    slots = halo_ref.shape[1]
    size = outs[0].shape[-1] // slots
    copies = []
    for d in range(len(OFFSETS)):
        for s in range(slots):
            start = pl.multiple_of(halo_ref[d, s, node_ref[0]] * size, size)
            copy = pltpu.make_async_copy(
                spectrum.at[:, :, pl.ds(start, size)],
                landed.at[d * slots + s],
                done.at[d * slots + s],
            )
            copy.start()
            copies.append(copy)
    for d in range(len(OFFSETS)):
        for s in range(slots):
            copies[d * slots + s].wait()
            outs[d][:, :, s * size : (s + 1) * size] = landed[d * slots + s].astype(
                outs[d].dtype
            )


def coupled_kernel(per_step, points, chunks, slot_ref, h_ref, *refs):
    owns = refs[: len(chunks)]
    halos = refs[len(chunks) : len(chunks) + len(OFFSETS)]
    (coupling, spectrum, source, capacitance, pulsation, ready, out, blocks) = refs[
        len(chunks) + len(OFFSETS) :
    ]
    rows = owns[0].shape[0]
    listed = coupling.shape[1]
    size = coupling.shape[2]
    slots = halos[0].shape[-1] // size
    count = blocks.shape[0] - len(OFFSETS) * slots - 1

    @pl.when(pl.program_id(0) == 0)
    def _():
        for (p, begin, wide), own in zip(chunks, owns):
            at = slice(p * rows, (p + 1) * rows)
            for b in range(wide // size):
                blocks[begin // size + b, at, :] = own[:, b * size : (b + 1) * size]
        for p in range(points):
            at = slice(p * rows, (p + 1) * rows)
            for d in range(len(OFFSETS)):
                for s in range(slots):
                    blocks[count + d * slots + s, at, :] = halos[d][
                        p, :, s * size : (s + 1) * size
                    ]
        blocks[count + len(OFFSETS) * slots] = jnp.zeros(blocks.shape[1:], blocks.dtype)

    even = lax.broadcasted_iota(jnp.int32, (rows, size), 0) % 2 == 0
    for b in range(per_step):
        entry = pl.program_id(0) * per_step + b
        left = jnp.concatenate([blocks[slot_ref[k, entry]] for k in range(listed)], axis=1)
        right = jnp.concatenate([coupling[b, k] for k in range(listed)], axis=1)
        total = lax.dot_general(
            left, right, (((1,), (1,)), ((), ())), preferred_element_type=jnp.float32
        )
        at = slice(b * size, (b + 1) * size)
        scale = pulsation[0] * capacitance[:, at]
        for p in range(points):
            values = spectrum[p, :, at]
            swapped = jnp.where(
                even, pltpu.roll(values, rows - 1, 0), pltpu.roll(values, 1, 0)
            )
            value = total[p * rows : (p + 1) * rows] + scale * swapped - source[p, :, at]
            out[p, :, at] = value + ready[0, :, at] if p == 0 else value


def nonlinear_kernel(parts, width, adds, h_ref, *refs):
    arrived = refs[:parts]
    (saturation, steepness, junction, synthesis, analysis) = refs[parts : parts + 5]
    (out, volt, samples) = refs[-3:]
    block = out.shape[-1]
    length = volt.shape[1]
    group = 16
    for turn, start in enumerate(range(0, block, width)):
        at = slice(start, start + width)
        slot = turn % 2
        spectra = jnp.concatenate(
            [ref[:, at] for ref in arrived], axis=0
        )
        volt[slot] = jnp.dot(synthesis[0], spectra, preferred_element_type=jnp.float32)
        steep = steepness[:, at]
        for row in range(0, length, group):
            here = slice(row, row + group)
            voltage = volt[slot, here, :]
            u = steep * voltage
            current = jnp.maximum(u, 0.0) + jnp.log(1.0 + jnp.exp(-jnp.abs(u))) - LOG_TWO
            samples[slot, here, :] = (saturation[:, at] * current).astype(jnp.bfloat16)
            charge = junction[:, at] * voltage * lax.rsqrt(1.0 + voltage * voltage)
            samples[slot, length + row : length + row + group, :] = charge.astype(jnp.bfloat16)
        total = jnp.dot(analysis[0], samples[slot], preferred_element_type=jnp.float32)
        out[0, :, at] = refs[parts + 5][0, :, at] + total if adds else total


def widest(total, unit, most):
    return max(w for w in range(unit, most + 1, unit) if total % w == 0)


def local(
    spectrum,
    source,
    coupling,
    capacitance,
    saturation,
    steepness,
    junction,
    halo_list,
    neighbour_slot,
):
    rows, points, nodes = spectrum.shape
    parts = lax.axis_size("harm")
    length = rows * parts
    count, listed, size, _ = coupling.shape
    slots = halo_list.shape[-1]
    harm = lax.axis_index("harm").astype(jnp.int32).reshape(1)
    synthesis, analysis, pulsation = tables(rows, parts)
    synthesis = jnp.asarray(synthesis, jnp.bfloat16)
    analysis = jnp.asarray(analysis, jnp.bfloat16)
    pulsation = jnp.asarray(pulsation, jnp.float32)

    by_point = spectrum.transpose(1, 0, 2)
    source_by_point = source.transpose(1, 0, 2)
    block = widest(nodes, LANES, 1536)
    chunks = [(p, 0, nodes) for p in range(points)]
    if nodes > block and points > 1:
        chunks[-1:] = [(points - 1, 0, nodes - block), (points - 1, nodes - block, block)]
    head = by_point[0].astype(jnp.bfloat16)
    later, _ = lax.optimization_barrier((by_point, head))
    owns = [head] + [
        later[p, :, begin : begin + wide].astype(jnp.bfloat16) for p, begin, wide in chunks[1:]
    ]
    after = lax.optimization_barrier((by_point, *owns))[0]
    arrived = [
        [own] + [passed_round(own, "harm", s) for s in range(1, parts)] for own in owns
    ]

    smem = pl.BlockSpec(memory_space=pltpu.SMEM)
    vmem = pl.BlockSpec(memory_space=pltpu.VMEM)
    packed = pl.pallas_call(
        pack_kernel,
        out_shape=[jax.ShapeDtypeStruct((points, rows, slots * size), jnp.bfloat16)]
        * len(OFFSETS),
        in_specs=[smem, smem, pl.BlockSpec(memory_space=pl.ANY)],
        out_specs=[vmem] * len(OFFSETS),
        scratch_shapes=[
            pltpu.VMEM((len(OFFSETS) * slots, points, rows, size), jnp.float32),
            pltpu.SemaphoreType.DMA((len(OFFSETS) * slots,)),
        ],
        name="pack",
    )(
        lax.axis_index("node").astype(jnp.int32).reshape(1),
        halo_list.transpose(1, 2, 0),
        after,
    )
    halos = [passed_along(value, "node", offset) for value, offset in zip(packed, OFFSETS)]

    width = widest(block, LANES, 256)

    def nonlinear(chunk, pair, added):
        p, begin, wide = chunk
        first = begin // block
        place = p if added is not None else 0
        shape = (points if added is not None else 1, rows, nodes)
        whole = pl.BlockSpec((1, rows, block), lambda i, h: (place, 0, i + first))
        scale = pl.BlockSpec((1, block), lambda i, h: (0, i + first))
        return pl.pallas_call(
            functools.partial(nonlinear_kernel, parts, width, added is not None),
            out_shape=jax.ShapeDtypeStruct(shape, jnp.float32),
            grid_spec=pltpu.PrefetchScalarGridSpec(
                num_scalar_prefetch=1,
                grid=(wide // block,),
                in_specs=[pl.BlockSpec((rows, block), lambda i, h: (0, i))] * parts
                + [scale] * 3
                + [
                    pl.BlockSpec((1, length, length), lambda i, h: (h[0], 0, 0)),
                    pl.BlockSpec((1, rows, 2 * length), lambda i, h: (h[0], 0, 0)),
                ]
                + ([whole] if added is not None else []),
                out_specs=whole,
                scratch_shapes=[
                    pltpu.VMEM((2, length, width), jnp.float32),
                    pltpu.VMEM((2, 2 * length, width), jnp.bfloat16),
                ],
            ),
            input_output_aliases={6 + parts: 0} if added is not None else {},
            cost_estimate=pl.CostEstimate(
                flops=2 * (length + 2 * rows) * length * wide,
                bytes_accessed=12 * rows * wide,
                transcendentals=3 * length * wide,
            ),
            name="nonlinear",
        )(
            harm,
            *pair,
            saturation.reshape(1, -1),
            steepness.reshape(1, -1),
            junction.reshape(1, -1),
            synthesis,
            analysis,
            *([added] if added is not None else []),
        )

    ready = nonlinear(chunks[0], arrived[0], None)

    per_step = widest(count, 1, 8)
    span = per_step * size
    base = pl.pallas_call(
        functools.partial(coupled_kernel, per_step, points, chunks),
        out_shape=jax.ShapeDtypeStruct((points, rows, nodes), jnp.float32),
        grid_spec=pltpu.PrefetchScalarGridSpec(
            num_scalar_prefetch=2,
            grid=(count // per_step,),
            in_specs=[pl.BlockSpec(own.shape, lambda i, n, h: (0, 0)) for own in owns]
            + [pl.BlockSpec((points, rows, slots * size), lambda i, n, h: (0, 0, 0))]
            * len(OFFSETS)
            + [
                pl.BlockSpec((per_step, listed, size, size), lambda i, n, h: (i, 0, 0, 0)),
                pl.BlockSpec((points, rows, span), lambda i, n, h: (0, 0, i)),
                pl.BlockSpec((points, rows, span), lambda i, n, h: (0, 0, i)),
                pl.BlockSpec((1, span), lambda i, n, h: (0, i)),
                pl.BlockSpec((1, rows, LANES), lambda i, n, h: (h[0], 0, 0)),
                pl.BlockSpec((1, rows, span), lambda i, n, h: (0, 0, i)),
            ],
            out_specs=pl.BlockSpec((points, rows, span), lambda i, n, h: (0, 0, i)),
            scratch_shapes=[
                pltpu.VMEM((count + len(OFFSETS) * slots + 1, points * rows, size), jnp.bfloat16)
            ],
        ),
        cost_estimate=pl.CostEstimate(
            flops=2 * points * rows * nodes * listed * size,
            bytes_accessed=coupling.size * 2 + spectrum.size * 14,
            transcendentals=0,
        ),
        name="coupled",
    )(
        neighbour_slot.T,
        harm,
        *owns,
        *halos,
        coupling,
        by_point,
        source_by_point,
        capacitance.reshape(1, -1),
        pulsation,
        ready,
    )

    result = base
    for chunk, pair in zip(chunks[1:], arrived[1:]):
        result = nonlinear(chunk, pair, result)
    return result.transpose(1, 0, 2)


def solution(mesh):
    in_specs = (
        P("harm", None, "node"),
        P("harm", None, "node"),
        P("node", None, None, None),
        P("node"),
        P("node"),
        P("node"),
        P("node"),
        P(),
        P("node", None),
    )
    out_specs = P("harm", None, "node")
    return jax.shard_map(local, mesh=mesh, in_specs=in_specs, out_specs=out_specs, check_vma=False)
```
